32 devices in a mesh: parts: 2 (over y), pix: 4 (over z), par: 4 (over x, core).
Axes of the slice: x: 2, y: 2, z: 4, core: 2. Of those that a mesh axis runs over, the one named last changes fastest.
Arguments:
- green_matrix: bfloat16 [4608, 16384], P('pix', 'par'), may hold values from -0.046875 to 0.046875
- observed: bfloat16 [64, 4608], P('parts', 'pix'), parts along dimension 0, may hold values from -1000 to 1000
Outputs:
- solution: float32 [64, 16384], P('parts', 'par'), parts along dimension 0
- residual: float32 [64, 4608], P('parts', 'pix'), parts along dimension 0
The draws below stay inside these ranges and needn't reach their ends.
There are 2 independent parts, one for each index of `parts`. The reference program is written for one: setup_inputs(seed, part) draws one part's arguments, and reference() takes and returns one part's arrays. A program takes and returns all parts, laid end to end along the dimension named above; an argument that names none is the same for every part. Nothing has to cross between parts.
All inputs are finite; a program needn't handle non-finite values.
Results may differ from the reference program's by a relative error of at most 0.0038.
Values may be sent and summed in bfloat16 or wider, within the bound.
A program may use at most 64 MiB of HBM per device.

```python
import math
import jax
import jax.numpy as jnp
from jax import lax

GRID = 128
PARAMS = 16384
SETS = 32
PIXELS = 4608
ITERS = 5


def draw_green_matrix(key, part):
    keys = jax.random.split(jax.random.fold_in(key, 29), 4)
    base = jnp.clip(jax.random.normal(keys[0], (PIXELS, PARAMS), jnp.float32), -6.0, 6.0)
    column_scale = jnp.exp(jax.random.uniform(keys[1], (1, PARAMS), jnp.float32, -2.5, 0.0))
    left = jax.random.normal(keys[2], (PIXELS, 3), jnp.float32)
    right = jax.random.normal(keys[3], (3, PARAMS), jnp.float32)
    common = left[:, 0:1] * right[0:1, :] + left[:, 1:2] * right[1:2, :] + left[:, 2:3] * right[2:3, :]
    common = common / math.sqrt(3.0)
    place = jnp.arange(PARAMS, dtype=jnp.float32)[None, :] / PARAMS - 1.0
    rising = jnp.exp(math.log(3.0) * place)
    value = (base + 0.06 * common) * column_scale * rising * (2.2 / GRID)
    bound = 6.0 / GRID
    return jnp.clip(value, -bound, bound).astype(jnp.bfloat16)


def draw_observed(key, part):
    keys = jax.random.split(jax.random.fold_in(key, 71), 3)
    position = jnp.arange(PIXELS, dtype=jnp.float32) / PIXELS
    base = jnp.clip(jax.random.normal(keys[0], (SETS, PIXELS), jnp.float32), -6.0, 6.0)
    rising = jnp.exp(math.log(3.0) * position)[None, :]
    row_scale = jnp.exp(jax.random.uniform(keys[1], (1, PIXELS), jnp.float32, math.log(0.5), math.log(5.0)))
    set_scale = jnp.exp(jax.random.uniform(keys[2], (SETS, 1), jnp.float32, math.log(0.3), math.log(3.0)))
    return (base * rising * row_scale * set_scale).astype(jnp.bfloat16)


def setup_inputs(seed: int = 0, part: int = 0) -> dict:
    seeds = jax.random.split(jax.random.key(seed), 3)
    own_keys = jax.random.split(jax.random.fold_in(seeds[2], part), 3)
    green_matrix = draw_green_matrix(jax.random.fold_in(seeds[2], 71), part)
    observed = draw_observed(jax.random.fold_in(jax.random.fold_in(seeds[2], part), 71), part)
    return {"green_matrix": green_matrix, "observed": observed}


def smooth(values):
    set_count = values.shape[0]
    tiles = values.reshape(set_count, GRID, GRID)
    padded = jnp.pad(tiles, ((0, 0), (1, 1), (1, 1)))
    beside_all = padded[:, 2:, 1:-1] + padded[:, :-2, 1:-1] + padded[:, 1:-1, 2:] + padded[:, 1:-1, :-2]
    return (0.25 * (4.0 * tiles - beside_all)).reshape(set_count, GRID * GRID)


def reference(green_matrix, observed):
    residual = observed.astype(jnp.float32)
    gradient = jnp.dot(observed, green_matrix, preferred_element_type=jnp.float32)
    grad_sq = jnp.sum(gradient * gradient, axis=1)
    direction = gradient
    solution = jnp.zeros((SETS, GRID * GRID), jnp.float32)
    smooth_res = jnp.zeros((SETS, GRID * GRID), jnp.float32)
    for sweep in range(ITERS):
        rounded = direction.astype(jnp.bfloat16)
        image = lax.dot_general(rounded, green_matrix, (((1,), (1,)), ((), ())), preferred_element_type=jnp.float32)
        smoothed = smooth(lax.optimization_barrier(rounded).astype(jnp.float32))
        curvature = jnp.sum(image * image, axis=1) + jnp.sum(smoothed * smoothed, axis=1)
        step_len = (grad_sq / curvature)[:, None]
        solution = solution + step_len * direction
        residual = residual - step_len * image
        smooth_res = smooth_res - step_len * smoothed
        if sweep + 1 < ITERS:
            gradient = jnp.dot(residual.astype(jnp.bfloat16), green_matrix, preferred_element_type=jnp.float32) + smooth(smooth_res)
            fresh_sq = jnp.sum(gradient * gradient, axis=1)
            direction = gradient + (fresh_sq / grad_sq)[:, None] * direction
            grad_sq = fresh_sq
    return solution, residual
```

```python
import functools

import jax
import jax.numpy as jnp
from jax import lax
from jax.experimental import pallas as pl
from jax.experimental.pallas import tpu as pltpu
from jax.sharding import PartitionSpec as P

GRID = 128
ITERS = 5
LANES = 128


def padded_2(block, sides, width):
    for axis, dim in sides:
        count = lax.axis_size(axis)
        forward = [(i, i + 1) for i in range(count - 1)]
        backward = [(target, source) for source, target in forward]
        low = lax.ppermute(
            lax.slice_in_dim(block, block.shape[dim] - width, None, axis=dim), axis, forward
        )
        high = lax.ppermute(lax.slice_in_dim(block, 0, width, axis=dim), axis, backward)
        block = jnp.concatenate([low, block, high], axis=dim)
    return block


def smooth(values):
    set_count = values.shape[0]
    grid_rows = values.shape[1] // GRID
    tiles = values.reshape(set_count, grid_rows, GRID)
    padded = padded_2(tiles, (("par", 1),), 1)
    padded = jnp.pad(padded, ((0, 0), (0, 0), (1, 1)))
    beside_all = (
        padded[:, 2:, 1:-1] + padded[:, :-2, 1:-1] + padded[:, 1:-1, 2:] + padded[:, 1:-1, :-2]
    )
    return (0.25 * (4.0 * tiles - beside_all)).reshape(set_count, grid_rows * GRID)


def forward(rounded, green_matrix):
    partial_value = lax.dot_general(
        rounded, green_matrix, (((1,), (1,)), ((), ())), preferred_element_type=jnp.float32
    )
    return lax.psum(partial_value, "par")


def curvatures(image, smoothed):
    local_image = jnp.sum(image * image, axis=1)
    local_smooth = jnp.sum(smoothed * smoothed, axis=1)
    image_sq = lax.psum(local_image, "pix")
    smooth_sq = lax.psum(local_smooth, "par")
    return image_sq + smooth_sq


def backward_sum(rounded, green_matrix):
    return lax.psum(jnp.dot(rounded, green_matrix, preferred_element_type=jnp.float32), "pix")


def column_squares(gradient):
    return lax.psum(jnp.sum(gradient * gradient, axis=1), "par")


def on_device(green_matrix, observed):
    set_count = observed.shape[0]
    tile_cells = green_matrix.shape[1]
    residual = observed.astype(jnp.float32)
    gradient = backward_sum(observed, green_matrix)
    grad_sq = column_squares(gradient)
    direction = gradient
    solution = jnp.zeros((set_count, tile_cells), jnp.float32)
    smooth_res = jnp.zeros((set_count, tile_cells), jnp.float32)
    for sweep in range(ITERS):
        rounded = direction.astype(jnp.bfloat16)
        image = forward(rounded, green_matrix)
        smoothed = smooth(lax.optimization_barrier(rounded).astype(jnp.float32))
        step_len = (grad_sq / curvatures(image, smoothed))[:, None]
        solution = solution + step_len * direction
        residual = residual - step_len * image
        smooth_res = smooth_res - step_len * smoothed
        if sweep + 1 < ITERS:
            gradient = backward_sum(residual.astype(jnp.bfloat16), green_matrix) + smooth(
                smooth_res
            )
            fresh_sq = column_squares(gradient)
            direction = gradient + (fresh_sq / grad_sq)[:, None] * direction
            grad_sq = fresh_sq
    return (solution, residual)


MESH = pl.DeviceIdType.MESH


def to_row(column):
    count = column.shape[0]
    eye = lax.broadcasted_iota(jnp.int32, (count, LANES), 0) == lax.broadcasted_iota(
        jnp.int32, (count, LANES), 1
    )
    return jnp.sum(jnp.where(eye, jnp.broadcast_to(column, (count, LANES)), 0.0), axis=0, keepdims=True)


def to_column(row, count):
    eye = lax.broadcasted_iota(jnp.int32, (count, LANES), 0) == lax.broadcasted_iota(
        jnp.int32, (count, LANES), 1
    )
    return jnp.sum(jnp.where(eye, jnp.broadcast_to(row, (count, LANES)), 0.0), axis=1, keepdims=True)


def stencil(above, here, below):
    lane = lax.broadcasted_iota(jnp.int32, here.shape, 1)
    left = jnp.where(lane == 0, 0.0, pltpu.roll(here, 1, 1))
    right = jnp.where(lane == GRID - 1, 0.0, pltpu.roll(here, GRID - 1, 1))
    return here - 0.25 * (above + below + left + right)


def cgls_kernel(
    nz, npar,
    green_hbm, obs_ref, x_ref, r_ref,
    green, imb, im, p_ext, sp, g_own, gg_ref,
    rs_send, rs_recv, ag, y_send, y_recv, h_recv, halo,
    sz, sp_scalar, nz_scalar, npar_scalar,
    load_sem, rs_ss, rs_rs, ag_ss, ag_rs, y_ss, y_rs, h_ss, h_rs, halo_ss, halo_rs,
    sz_ss, sz_rs, sp_ss, sp_rs, nz_ss, nz_rs, np_ss, np_rs,
):
    me_z = lax.axis_index("pix")
    me_p = lax.axis_index("par")
    core = lax.rem(me_p, 2)
    chip = me_p // 2
    nchip = npar // 2
    partner = me_p + 1 - 2 * core
    sets = obs_ref.shape[0]
    half = sets // 2
    width = green.shape[2]
    rows = nz * width // GRID
    own_rows = width // GRID
    edge = 2 * GRID

    loads = [
        pltpu.make_async_copy(green_hbm.at[:, pl.ds(c * width, width)], green.at[c], load_sem.at[c])
        for c in range(nz)
    ]
    for c in range(nz):
        loads[c].start()

    barrier = pltpu.get_barrier_semaphore()
    for j in range(1, nz):
        pl.semaphore_signal(barrier, inc=1, device_id={"pix": lax.rem(me_z + j, nz)}, device_id_type=MESH)
    for j in range(1, npar):
        pl.semaphore_signal(barrier, inc=1, device_id={"par": lax.rem(me_p + j, npar)}, device_id_type=MESH)

    imb[...] = obs_ref[...]
    im[...] = jnp.zeros_like(im)
    p_ext[...] = jnp.zeros_like(p_ext)
    g_own[...] = jnp.zeros_like(g_own)
    gg_ref[...] = jnp.zeros_like(gg_ref)
    x_ref[...] = jnp.zeros_like(x_ref)
    r_ref[...] = obs_ref[...].astype(jnp.float32)

    pl.semaphore_wait(barrier, nz + npar - 2)
    for c in range(nz):
        loads[c].wait()

    def to_z(buf, k, ssem, rsem, peer):
        return pltpu.make_async_remote_copy(
            src_ref=buf.at[k, me_z], dst_ref=buf.at[k, me_z],
            send_sem=ssem.at[k, peer], recv_sem=rsem.at[k, me_z],
            device_id={"pix": peer}, device_id_type=MESH,
        )

    def from_z(buf, k, ssem, rsem, peer):
        return pltpu.make_async_remote_copy(
            src_ref=buf.at[k, peer], dst_ref=buf.at[k, peer],
            send_sem=ssem.at[k, peer], recv_sem=rsem.at[k, peer],
            device_id={"pix": peer}, device_id_type=MESH,
        )

    def to_par(buf, k, ssem, rsem, peer):
        return pltpu.make_async_remote_copy(
            src_ref=buf.at[k, me_p], dst_ref=buf.at[k, me_p],
            send_sem=ssem.at[k, peer], recv_sem=rsem.at[k, me_p],
            device_id={"par": peer}, device_id_type=MESH,
        )

    def from_par(buf, k, ssem, rsem, peer):
        return pltpu.make_async_remote_copy(
            src_ref=buf.at[k, peer], dst_ref=buf.at[k, peer],
            send_sem=ssem.at[k, peer], recv_sem=rsem.at[k, peer],
            device_id={"par": peer}, device_id_type=MESH,
        )

    z_peers = [lax.rem(me_z + j, nz) for j in range(1, nz)]
    z_from = [lax.rem(me_z + nz - j, nz) for j in range(1, nz)]
    p_peers = [lax.rem(me_p + j, npar) for j in range(1, npar)]

    def total_row(buf, k, count):
        value = buf[k, 0, 0:1]
        for i in range(1, count):
            value = value + buf[k, i, 0:1]
        return value

    def send_image_sq(k):
        image = im[...]
        row = to_row(jnp.sum(image * image, axis=1, keepdims=True))
        sz[k, me_z] = jnp.broadcast_to(row, (8, LANES))
        for peer in z_peers:
            to_z(sz, k, sz_ss, sz_rs, peer).start()

    def send_smooth_sq(k):
        square = jnp.zeros((sets, GRID), jnp.float32)
        for i in range(rows + 2):
            line = stencil(
                p_ext[:, i * GRID:(i + 1) * GRID],
                p_ext[:, (i + 1) * GRID:(i + 2) * GRID],
                p_ext[:, (i + 2) * GRID:(i + 3) * GRID],
            )
            if i == 0:
                line = jnp.where(me_p == 0, 0.0, line)
            elif i == rows + 1:
                line = jnp.where(me_p == npar - 1, 0.0, line)
            else:
                square = square + line * line
            sp[:, i * GRID:(i + 1) * GRID] = line
        row = to_row(jnp.sum(square, axis=1, keepdims=True))
        sp_scalar[k, me_p] = jnp.broadcast_to(row, (8, LANES))
        for peer in p_peers:
            to_par(sp_scalar, k, sp_ss, sp_rs, peer).start()

    def curvature(k):
        for peer in p_peers:
            from_par(sp_scalar, k, sp_ss, sp_rs, peer).wait_recv()
        for peer in z_from:
            from_z(sz, k, sz_ss, sz_rs, peer).wait_recv()
        return total_row(sz, k, nz) + total_row(sp_scalar, k, npar)

    def apply_step(step):
        x_ref[...] += step * p_ext[:, edge:edge + rows * GRID]
        r_ref[...] -= step * im[...]

    def finish_scalars(k):
        for peer in z_peers:
            to_z(sz, k, sz_ss, sz_rs, peer).wait_send()
        for peer in p_peers:
            to_par(sp_scalar, k, sp_ss, sp_rs, peer).wait_send()

    def rs_copy(k, target):
        return pltpu.make_async_remote_copy(
            src_ref=rs_send.at[k, target], dst_ref=rs_recv.at[k, me_z],
            send_sem=rs_ss.at[k, target], recv_sem=rs_rs.at[k, me_z],
            device_id={"pix": target}, device_id_type=MESH,
        )

    def rs_from(k, source):
        return pltpu.make_async_remote_copy(
            src_ref=rs_send.at[k, source], dst_ref=rs_recv.at[k, source],
            send_sem=rs_ss.at[k, source], recv_sem=rs_rs.at[k, source],
            device_id={"pix": source}, device_id_type=MESH,
        )

    up = lax.rem(me_p + 1, npar)
    down = lax.rem(me_p + npar - 1, npar)

    def halo_copies(k):
        return (
            pltpu.make_async_remote_copy(
                src_ref=ag.at[k, nz - 1, :, pl.ds(width - edge, edge)], dst_ref=halo.at[k, 0],
                send_sem=halo_ss.at[k, 0], recv_sem=halo_rs.at[k, 0],
                device_id={"par": up}, device_id_type=MESH,
            ),
            pltpu.make_async_remote_copy(
                src_ref=ag.at[k, 0, :, pl.ds(0, edge)], dst_ref=halo.at[k, 1],
                send_sem=halo_ss.at[k, 1], recv_sem=halo_rs.at[k, 1],
                device_id={"par": down}, device_id_type=MESH,
            ),
        )

    def y_copy(k):
        return pltpu.make_async_remote_copy(
            src_ref=y_send.at[k], dst_ref=y_recv.at[k],
            send_sem=y_ss.at[k], recv_sem=y_rs.at[k],
            device_id={"par": partner}, device_id_type=MESH,
        )

    @pl.loop(0, ITERS)
    def _(k):
        send_image_sq(k)
        vector = imb[...]
        for peer in z_peers:
            rs_send[k, peer] = jnp.dot(
                vector, green[peer], preferred_element_type=jnp.float32
            ).astype(jnp.bfloat16)
            rs_copy(k, peer).start()
        send_smooth_sq(k)
        fresh = jnp.dot(vector, green[me_z], preferred_element_type=jnp.float32)
        base = me_z * own_rows
        lines = []
        for i in range(own_rows):
            lines.append(stencil(*[
                sp[:, pl.ds(pl.multiple_of((base + i + d) * GRID, GRID), GRID)] for d in range(3)
            ]))
        fresh = fresh + jnp.concatenate(lines, axis=1)
        step = jnp.where(k == 0, -1.0, gg_ref[0:1] / curvature(k))
        step = to_column(step, sets)
        apply_step(step)
        for source in z_from:
            rs_from(k, source).wait_recv()
            fresh = fresh + rs_recv[k, source].astype(jnp.float32)
        gradient = g_own[...] - step * fresh
        g_own[...] = gradient
        ag[k, me_z] = gradient.astype(jnp.bfloat16)
        for peer in z_peers:
            to_z(ag, k, ag_ss, ag_rs, peer).start()
        row = to_row(jnp.sum(gradient * gradient, axis=1, keepdims=True))
        nz_scalar[k, me_z] = jnp.broadcast_to(row, (8, LANES))
        for peer in z_peers:
            to_z(nz_scalar, k, nz_ss, nz_rs, peer).start()

        def forward(index):
            return lax.dot_general(
                ag[k, index], green[index], (((1,), (1,)), ((), ())),
                preferred_element_type=jnp.float32,
            )

        image = forward(me_z)
        for source in z_from:
            from_z(ag, k, ag_ss, ag_rs, source).wait_recv()
            image = image + forward(source)
        for source in z_from:
            from_z(nz_scalar, k, nz_ss, nz_rs, source).wait_recv()
        low, high = image[:half], image[half:]
        mine = jnp.where(core == 0, low, high)
        y_send[k] = jnp.where(core == 0, high, low).astype(jnp.bfloat16)
        y_copy(k).start()
        npar_scalar[k, me_p] = jnp.broadcast_to(total_row(nz_scalar, k, nz), (8, LANES))
        for peer in p_peers:
            to_par(npar_scalar, k, np_ss, np_rs, peer).start()
        for copy in halo_copies(k):
            copy.start()
        y_copy(k).wait_recv()
        h_recv[k, me_p] = (mine + y_recv[k].astype(jnp.float32)).astype(jnp.bfloat16)
        for peer in p_peers:
            to_par(h_recv, k, h_ss, h_rs, peer).start()

        for peer in p_peers:
            from_par(npar_scalar, k, np_ss, np_rs, peer).wait_recv()
        fresh_sq = total_row(npar_scalar, k, npar)
        ratio = to_column(jnp.where(k == 0, 0.0, fresh_sq / gg_ref[0:1]), sets)
        gg_ref[...] = jnp.broadcast_to(fresh_sq, gg_ref.shape)
        for copy in halo_copies(k):
            copy.wait_recv()
        for c in range(nz):
            where = slice(edge + c * width, edge + (c + 1) * width)
            p_ext[:, where] = ag[k, c].astype(jnp.float32) + ratio * p_ext[:, where]
        first = jnp.where(me_p == 0, 0.0, halo[k, 0].astype(jnp.float32))
        p_ext[:, :edge] = first + ratio * p_ext[:, :edge]
        last = jnp.where(me_p == npar - 1, 0.0, halo[k, 1].astype(jnp.float32))
        p_ext[:, edge + rows * GRID:] = last + ratio * p_ext[:, edge + rows * GRID:]

        for peer in p_peers:
            from_par(h_recv, k, h_ss, h_rs, peer).wait_recv()
        for c in range(2):
            part = h_recv[k, c].astype(jnp.float32)
            for i in range(1, nchip):
                part = part + h_recv[k, 2 * i + c].astype(jnp.float32)
            where = slice(c * half, (c + 1) * half)
            im[where] = part + ratio[where] * im[where]
        imb[...] = im[...].astype(jnp.bfloat16)

        finish_scalars(k)
        for peer in z_peers:
            rs_copy(k, peer).wait_send()
            to_z(ag, k, ag_ss, ag_rs, peer).wait_send()
            to_z(nz_scalar, k, nz_ss, nz_rs, peer).wait_send()
        y_copy(k).wait_send()
        for copy in halo_copies(k):
            copy.wait_send()
        for peer in p_peers:
            to_par(npar_scalar, k, np_ss, np_rs, peer).wait_send()
            to_par(h_recv, k, h_ss, h_rs, peer).wait_send()

    send_image_sq(ITERS)
    send_smooth_sq(ITERS)
    step = to_column(gg_ref[0:1] / curvature(ITERS), sets)
    apply_step(step)
    finish_scalars(ITERS)


def on_device_kernel(nz, npar, green_matrix, observed):
    sets, pixels = observed.shape
    cells = green_matrix.shape[1]
    width = cells // nz
    half = sets // 2
    bf16, f32 = jnp.bfloat16, jnp.float32
    dma = pltpu.SemaphoreType.DMA
    n = ITERS
    vmem = pl.BlockSpec(memory_space=pltpu.VMEM)
    return pl.pallas_call(
        functools.partial(cgls_kernel, nz, npar),
        out_shape=(
            jax.ShapeDtypeStruct((sets, cells), f32),
            jax.ShapeDtypeStruct((sets, pixels), f32),
        ),
        in_specs=[pl.BlockSpec(memory_space=pl.ANY), vmem],
        out_specs=(vmem, vmem),
        scratch_shapes=[
            pltpu.VMEM((nz, pixels, width), bf16),
            pltpu.VMEM((sets, pixels), bf16),
            pltpu.VMEM((sets, pixels), f32),
            pltpu.VMEM((sets, cells + 4 * GRID), f32),
            pltpu.VMEM((sets, cells + 2 * GRID), f32),
            pltpu.VMEM((sets, width), f32),
            pltpu.VMEM((8, LANES), f32),
            pltpu.VMEM((n, nz, sets, width), bf16),
            pltpu.VMEM((n, nz, sets, width), bf16),
            pltpu.VMEM((n, nz, sets, width), bf16),
            pltpu.VMEM((n, half, pixels), bf16),
            pltpu.VMEM((n, half, pixels), bf16),
            pltpu.VMEM((n, npar, half, pixels), bf16),
            pltpu.VMEM((n, 2, sets, 2 * GRID), bf16),
            pltpu.VMEM((n + 1, nz, 8, LANES), f32),
            pltpu.VMEM((n + 1, npar, 8, LANES), f32),
            pltpu.VMEM((n, nz, 8, LANES), f32),
            pltpu.VMEM((n, npar, 8, LANES), f32),
            dma((nz,)),
            dma((n, nz)), dma((n, nz)),
            dma((n, nz)), dma((n, nz)),
            dma((n,)), dma((n,)),
            dma((n, npar)), dma((n, npar)),
            dma((n, 2)), dma((n, 2)),
            dma((n + 1, nz)), dma((n + 1, nz)),
            dma((n + 1, npar)), dma((n + 1, npar)),
            dma((n, nz)), dma((n, nz)),
            dma((n, npar)), dma((n, npar)),
        ],
        compiler_params=pltpu.CompilerParams(
            collective_id=0, has_side_effects=True, vmem_limit_bytes=60 * 1024 * 1024
        ),
    )(green_matrix, observed)


def solution(mesh):
    nz, npar = mesh.shape["pix"], mesh.shape["par"]

    def step(green_matrix, observed):
        sets, cells = observed.shape[0], green_matrix.shape[1]
        fits = cells % (nz * GRID) == 0 and cells // nz >= 2 * GRID
        if fits and nz > 1 and npar % 2 == 0 and sets % 32 == 0 and sets <= LANES:
            return on_device_kernel(nz, npar, green_matrix, observed)
        return on_device(green_matrix, observed)

    return jax.shard_map(
        step,
        mesh=mesh,
        in_specs=(P("pix", "par"), P("parts", "pix")),
        out_specs=(P("parts", "par"), P("parts", "pix")),
        check_vma=False,
    )
```

```python
import functools

import jax
import jax.numpy as jnp
from jax import lax
from jax.experimental import pallas as pl
from jax.experimental.pallas import tpu as pltpu
from jax.sharding import PartitionSpec as P

GRID = 128
ITERS = 5
LANES = 128
SUB = 2


def padded_2(block, sides, width):
    for axis, dim in sides:
        count = lax.axis_size(axis)
        forward = [(i, i + 1) for i in range(count - 1)]
        backward = [(target, source) for source, target in forward]
        low = lax.ppermute(
            lax.slice_in_dim(block, block.shape[dim] - width, None, axis=dim), axis, forward
        )
        high = lax.ppermute(lax.slice_in_dim(block, 0, width, axis=dim), axis, backward)
        block = jnp.concatenate([low, block, high], axis=dim)
    return block


def smooth(values):
    set_count = values.shape[0]
    grid_rows = values.shape[1] // GRID
    tiles = values.reshape(set_count, grid_rows, GRID)
    padded = padded_2(tiles, (("par", 1),), 1)
    padded = jnp.pad(padded, ((0, 0), (0, 0), (1, 1)))
    beside_all = (
        padded[:, 2:, 1:-1] + padded[:, :-2, 1:-1] + padded[:, 1:-1, 2:] + padded[:, 1:-1, :-2]
    )
    return (0.25 * (4.0 * tiles - beside_all)).reshape(set_count, grid_rows * GRID)


def forward(rounded, green_matrix):
    partial_value = lax.dot_general(
        rounded, green_matrix, (((1,), (1,)), ((), ())), preferred_element_type=jnp.float32
    )
    return lax.psum(partial_value, "par")


def curvatures(image, smoothed):
    local_image = jnp.sum(image * image, axis=1)
    local_smooth = jnp.sum(smoothed * smoothed, axis=1)
    image_sq = lax.psum(local_image, "pix")
    smooth_sq = lax.psum(local_smooth, "par")
    return image_sq + smooth_sq


def backward_sum(rounded, green_matrix):
    return lax.psum(jnp.dot(rounded, green_matrix, preferred_element_type=jnp.float32), "pix")


def column_squares(gradient):
    return lax.psum(jnp.sum(gradient * gradient, axis=1), "par")


def on_device(green_matrix, observed):
    set_count = observed.shape[0]
    tile_cells = green_matrix.shape[1]
    residual = observed.astype(jnp.float32)
    gradient = backward_sum(observed, green_matrix)
    grad_sq = column_squares(gradient)
    direction = gradient
    solution = jnp.zeros((set_count, tile_cells), jnp.float32)
    smooth_res = jnp.zeros((set_count, tile_cells), jnp.float32)
    for sweep in range(ITERS):
        rounded = direction.astype(jnp.bfloat16)
        image = forward(rounded, green_matrix)
        smoothed = smooth(lax.optimization_barrier(rounded).astype(jnp.float32))
        step_len = (grad_sq / curvatures(image, smoothed))[:, None]
        solution = solution + step_len * direction
        residual = residual - step_len * image
        smooth_res = smooth_res - step_len * smoothed
        if sweep + 1 < ITERS:
            gradient = backward_sum(residual.astype(jnp.bfloat16), green_matrix) + smooth(
                smooth_res
            )
            fresh_sq = column_squares(gradient)
            direction = gradient + (fresh_sq / grad_sq)[:, None] * direction
            grad_sq = fresh_sq
    return (solution, residual)


MESH = pl.DeviceIdType.MESH


def to_row(column):
    count = column.shape[0]
    eye = lax.broadcasted_iota(jnp.int32, (count, LANES), 0) == lax.broadcasted_iota(
        jnp.int32, (count, LANES), 1
    )
    return jnp.sum(jnp.where(eye, jnp.broadcast_to(column, (count, LANES)), 0.0), axis=0, keepdims=True)


def to_column(row, count):
    eye = lax.broadcasted_iota(jnp.int32, (count, LANES), 0) == lax.broadcasted_iota(
        jnp.int32, (count, LANES), 1
    )
    return jnp.sum(jnp.where(eye, jnp.broadcast_to(row, (count, LANES)), 0.0), axis=1, keepdims=True)


def flipped(index, mask, count):
    value, bit = 0, 1
    while bit < count:
        digit = lax.rem(index // bit, 2)
        value = value + bit * (1 - digit if mask & bit else digit)
        bit *= 2
    return value


def far_first(count):
    masks = []
    bit = count // 2
    while bit:
        masks += range(bit, 2 * bit)
        bit //= 2
    return masks


def stencil(above, here, below):
    lane = lax.broadcasted_iota(jnp.int32, here.shape, 1)
    left = jnp.where(lane == 0, 0.0, pltpu.roll(here, 1, 1))
    right = jnp.where(lane == GRID - 1, 0.0, pltpu.roll(here, GRID - 1, 1))
    return here - 0.25 * (above + below + left + right)


def cgls_kernel(
    nz, npar,
    green_hbm, obs_ref, x_ref, r_ref,
    green, imb, im, p_ext, sp, g_own, own_part, gg_ref,
    rs_send, rs_recv, ag, y_send, y_recv, h_recv, halo,
    sz, sp_scalar, nz_scalar, npar_scalar,
    load_sem, rs_ss, rs_rs, ag_ss, ag_rs, y_ss, y_rs, h_ss, h_rs, halo_ss, halo_rs,
    sz_ss, sz_rs, sp_ss, sp_rs, nz_ss, nz_rs, np_ss, np_rs,
):
    me_z = lax.axis_index("pix")
    me_p = lax.axis_index("par")
    core = lax.rem(me_p, 2)
    chip = me_p // 2
    nchip = npar // 2
    partner = me_p + 1 - 2 * core
    sets = obs_ref.shape[0]
    half = sets // 2
    width = green.shape[3]
    rows = nz * SUB * width // GRID
    own_rows = width // GRID
    edge = 2 * GRID
    z_peers = [flipped(me_z, mask, nz) for mask in far_first(nz)]
    z_from = z_peers[::-1]
    p_peers = [lax.rem(me_p + j, npar) for j in range(1, npar)]
    order = [(s, c) for s in range(SUB) for c in z_peers] + [(s, me_z) for s in range(SUB)]

    def load(s, c):
        first = pl.multiple_of((c * SUB + s) * width, width)
        return pltpu.make_async_copy(
            green_hbm.at[:, pl.ds(first, width)], green.at[c, s], load_sem.at[c, s]
        )

    for s, c in order:
        load(s, c).start()

    barrier = pltpu.get_barrier_semaphore()
    for j in range(1, nz):
        pl.semaphore_signal(barrier, inc=1, device_id={"pix": lax.rem(me_z + j, nz)}, device_id_type=MESH)
    for j in range(1, npar):
        pl.semaphore_signal(barrier, inc=1, device_id={"par": lax.rem(me_p + j, npar)}, device_id_type=MESH)

    imb[...] = obs_ref[...]
    im[...] = jnp.zeros_like(im)
    p_ext[...] = jnp.zeros_like(p_ext)
    g_own[...] = jnp.zeros_like(g_own)
    gg_ref[...] = jnp.zeros_like(gg_ref)
    x_ref[...] = jnp.zeros_like(x_ref)
    r_ref[...] = obs_ref[...].astype(jnp.float32)

    pl.semaphore_wait(barrier, nz + npar - 2)

    def to_z(buf, k, ssem, rsem, peer, s=0):
        return pltpu.make_async_remote_copy(
            src_ref=buf.at[k, me_z, s], dst_ref=buf.at[k, me_z, s],
            send_sem=ssem.at[k, peer, s], recv_sem=rsem.at[k, me_z, s],
            device_id={"pix": peer}, device_id_type=MESH,
        )

    def from_z(buf, k, ssem, rsem, peer, s=0):
        return pltpu.make_async_remote_copy(
            src_ref=buf.at[k, peer, s], dst_ref=buf.at[k, peer, s],
            send_sem=ssem.at[k, peer, s], recv_sem=rsem.at[k, peer, s],
            device_id={"pix": peer}, device_id_type=MESH,
        )

    def to_par(buf, k, ssem, rsem, peer):
        return pltpu.make_async_remote_copy(
            src_ref=buf.at[k, me_p], dst_ref=buf.at[k, me_p],
            send_sem=ssem.at[k, peer], recv_sem=rsem.at[k, me_p],
            device_id={"par": peer}, device_id_type=MESH,
        )

    def from_par(buf, k, ssem, rsem, peer):
        return pltpu.make_async_remote_copy(
            src_ref=buf.at[k, peer], dst_ref=buf.at[k, peer],
            send_sem=ssem.at[k, peer], recv_sem=rsem.at[k, peer],
            device_id={"par": peer}, device_id_type=MESH,
        )


    def total_row(parts):
        value = parts[0]
        for part in parts[1:]:
            value = value + part
        return value

    def z_row(buf, k):
        return total_row([buf[k, i, 0, 0:1] for i in range(nz)])

    def par_row(buf, k):
        return total_row([buf[k, i, 0:1] for i in range(npar)])

    def send_image_sq(k):
        image = im[...]
        row = to_row(jnp.sum(image * image, axis=1, keepdims=True))
        sz[k, me_z, 0] = jnp.broadcast_to(row, (8, LANES))
        for peer in z_peers:
            to_z(sz, k, sz_ss, sz_rs, peer).start()

    def send_smooth_sq(k):
        square = jnp.zeros((sets, GRID), jnp.float32)
        for i in range(rows + 2):
            line = stencil(
                p_ext[:, i * GRID:(i + 1) * GRID],
                p_ext[:, (i + 1) * GRID:(i + 2) * GRID],
                p_ext[:, (i + 2) * GRID:(i + 3) * GRID],
            )
            if i == 0:
                line = jnp.where(me_p == 0, 0.0, line)
            elif i == rows + 1:
                line = jnp.where(me_p == npar - 1, 0.0, line)
            else:
                square = square + line * line
            sp[:, i * GRID:(i + 1) * GRID] = line
        row = to_row(jnp.sum(square, axis=1, keepdims=True))
        sp_scalar[k, me_p] = jnp.broadcast_to(row, (8, LANES))
        for peer in p_peers:
            to_par(sp_scalar, k, sp_ss, sp_rs, peer).start()

    def curvature(k):
        for peer in p_peers:
            from_par(sp_scalar, k, sp_ss, sp_rs, peer).wait_recv()
        for peer in z_from:
            from_z(sz, k, sz_ss, sz_rs, peer).wait_recv()
        return z_row(sz, k) + par_row(sp_scalar, k)

    def apply_step(step):
        x_ref[...] += step * p_ext[:, edge:edge + rows * GRID]
        r_ref[...] -= step * im[...]

    def finish_scalars(k):
        for peer in z_peers:
            to_z(sz, k, sz_ss, sz_rs, peer).wait_send()
        for peer in p_peers:
            to_par(sp_scalar, k, sp_ss, sp_rs, peer).wait_send()

    def rs_copy(k, target, s):
        return pltpu.make_async_remote_copy(
            src_ref=rs_send.at[k, target, s], dst_ref=rs_recv.at[k, me_z, s],
            send_sem=rs_ss.at[k, target, s], recv_sem=rs_rs.at[k, me_z, s],
            device_id={"pix": target}, device_id_type=MESH,
        )

    def rs_from(k, source, s):
        return pltpu.make_async_remote_copy(
            src_ref=rs_send.at[k, source, s], dst_ref=rs_recv.at[k, source, s],
            send_sem=rs_ss.at[k, source, s], recv_sem=rs_rs.at[k, source, s],
            device_id={"pix": source}, device_id_type=MESH,
        )

    up = lax.rem(me_p + 1, npar)
    down = lax.rem(me_p + npar - 1, npar)

    def halo_copies(k):
        return (
            pltpu.make_async_remote_copy(
                src_ref=ag.at[k, nz - 1, SUB - 1, :, pl.ds(width - edge, edge)], dst_ref=halo.at[k, 0],
                send_sem=halo_ss.at[k, 0], recv_sem=halo_rs.at[k, 0],
                device_id={"par": up}, device_id_type=MESH,
            ),
            pltpu.make_async_remote_copy(
                src_ref=ag.at[k, 0, 0, :, pl.ds(0, edge)], dst_ref=halo.at[k, 1],
                send_sem=halo_ss.at[k, 1], recv_sem=halo_rs.at[k, 1],
                device_id={"par": down}, device_id_type=MESH,
            ),
        )

    def y_copy(k):
        return pltpu.make_async_remote_copy(
            src_ref=y_send.at[k], dst_ref=y_recv.at[k],
            send_sem=y_ss.at[k], recv_sem=y_rs.at[k],
            device_id={"par": partner}, device_id_type=MESH,
        )

    @pl.loop(0, ITERS)
    def _(k):
        send_image_sq(k)
        vector = imb[...]

        def backward(s, c):
            @pl.when(k == 0)
            def _():
                load(s, c).wait()

            return jnp.dot(vector, green[c, s], preferred_element_type=jnp.float32)

        for s in range(SUB):
            for peer in z_peers:
                rs_send[k, peer, s] = backward(s, peer).astype(jnp.bfloat16)
                rs_copy(k, peer, s).start()
        send_smooth_sq(k)
        for s in range(SUB):
            base = (me_z * SUB + s) * own_rows
            lines = []
            for i in range(own_rows):
                lines.append(stencil(*[
                    sp[:, pl.ds(pl.multiple_of((base + i + d) * GRID, GRID), GRID)]
                    for d in range(3)
                ]))
            own_part[s] = backward(s, me_z) + jnp.concatenate(lines, axis=1)
        step = jnp.where(k == 0, -1.0, gg_ref[0:1] / curvature(k))
        step = to_column(step, sets)
        square = jnp.zeros((sets, 1), jnp.float32)
        for s in range(SUB):
            fresh = own_part[s]
            for source in z_from:
                rs_from(k, source, s).wait_recv()
                fresh = fresh + rs_recv[k, source, s].astype(jnp.float32)
            gradient = g_own[s] - step * fresh
            g_own[s] = gradient
            ag[k, me_z, s] = gradient.astype(jnp.bfloat16)
            for peer in z_peers:
                to_z(ag, k, ag_ss, ag_rs, peer, s).start()
            square = square + jnp.sum(gradient * gradient, axis=1, keepdims=True)
        nz_scalar[k, me_z, 0] = jnp.broadcast_to(to_row(square), (8, LANES))
        for peer in z_peers:
            to_z(nz_scalar, k, nz_ss, nz_rs, peer).start()
        apply_step(step)

        def forward(s, c):
            return lax.dot_general(
                ag[k, c, s], green[c, s], (((1,), (1,)), ((), ())),
                preferred_element_type=jnp.float32,
            )

        image = jnp.zeros(im.shape, jnp.float32)
        for s in range(SUB):
            image = image + forward(s, me_z)
        for s in range(SUB):
            for source in z_from:
                from_z(ag, k, ag_ss, ag_rs, source, s).wait_recv()
                image = image + forward(s, source)
        for source in z_from:
            from_z(nz_scalar, k, nz_ss, nz_rs, source).wait_recv()
        low, high = image[:half], image[half:]
        mine = jnp.where(core == 0, low, high)
        y_send[k] = jnp.where(core == 0, high, low).astype(jnp.bfloat16)
        y_copy(k).start()
        npar_scalar[k, me_p] = jnp.broadcast_to(z_row(nz_scalar, k), (8, LANES))
        for peer in p_peers:
            to_par(npar_scalar, k, np_ss, np_rs, peer).start()
        for copy in halo_copies(k):
            copy.start()
        y_copy(k).wait_recv()
        h_recv[k, me_p] = (mine + y_recv[k].astype(jnp.float32)).astype(jnp.bfloat16)
        for peer in p_peers:
            to_par(h_recv, k, h_ss, h_rs, peer).start()

        for peer in p_peers:
            from_par(npar_scalar, k, np_ss, np_rs, peer).wait_recv()
        fresh_sq = par_row(npar_scalar, k)
        ratio = to_column(jnp.where(k == 0, 0.0, fresh_sq / gg_ref[0:1]), sets)
        gg_ref[...] = jnp.broadcast_to(fresh_sq, gg_ref.shape)
        for copy in halo_copies(k):
            copy.wait_recv()
        for c in range(nz):
            for s in range(SUB):
                first = edge + (c * SUB + s) * width
                where = slice(first, first + width)
                p_ext[:, where] = ag[k, c, s].astype(jnp.float32) + ratio * p_ext[:, where]
        first = jnp.where(me_p == 0, 0.0, halo[k, 0].astype(jnp.float32))
        p_ext[:, :edge] = first + ratio * p_ext[:, :edge]
        last = jnp.where(me_p == npar - 1, 0.0, halo[k, 1].astype(jnp.float32))
        p_ext[:, edge + rows * GRID:] = last + ratio * p_ext[:, edge + rows * GRID:]

        for peer in p_peers:
            from_par(h_recv, k, h_ss, h_rs, peer).wait_recv()
        for c in range(2):
            part = h_recv[k, c].astype(jnp.float32)
            for i in range(1, nchip):
                part = part + h_recv[k, 2 * i + c].astype(jnp.float32)
            where = slice(c * half, (c + 1) * half)
            im[where] = part + ratio[where] * im[where]
        imb[...] = im[...].astype(jnp.bfloat16)

        finish_scalars(k)
        for peer in z_peers:
            for s in range(SUB):
                rs_copy(k, peer, s).wait_send()
                to_z(ag, k, ag_ss, ag_rs, peer, s).wait_send()
            to_z(nz_scalar, k, nz_ss, nz_rs, peer).wait_send()
        y_copy(k).wait_send()
        for copy in halo_copies(k):
            copy.wait_send()
        for peer in p_peers:
            to_par(npar_scalar, k, np_ss, np_rs, peer).wait_send()
            to_par(h_recv, k, h_ss, h_rs, peer).wait_send()

    send_image_sq(ITERS)
    send_smooth_sq(ITERS)
    step = to_column(gg_ref[0:1] / curvature(ITERS), sets)
    apply_step(step)
    finish_scalars(ITERS)


def on_device_kernel(nz, npar, green_matrix, observed):
    sets, pixels = observed.shape
    cells = green_matrix.shape[1]
    width = cells // (nz * SUB)
    half = sets // 2
    bf16, f32 = jnp.bfloat16, jnp.float32
    dma = pltpu.SemaphoreType.DMA
    n = ITERS
    vmem = pl.BlockSpec(memory_space=pltpu.VMEM)
    return pl.pallas_call(
        functools.partial(cgls_kernel, nz, npar),
        out_shape=(
            jax.ShapeDtypeStruct((sets, cells), f32),
            jax.ShapeDtypeStruct((sets, pixels), f32),
        ),
        in_specs=[pl.BlockSpec(memory_space=pl.ANY), vmem],
        out_specs=(vmem, vmem),
        scratch_shapes=[
            pltpu.VMEM((nz, SUB, pixels, width), bf16),
            pltpu.VMEM((sets, pixels), bf16),
            pltpu.VMEM((sets, pixels), f32),
            pltpu.VMEM((sets, cells + 4 * GRID), f32),
            pltpu.VMEM((sets, cells + 2 * GRID), f32),
            pltpu.VMEM((SUB, sets, width), f32),
            pltpu.VMEM((SUB, sets, width), f32),
            pltpu.VMEM((8, LANES), f32),
            pltpu.VMEM((n, nz, SUB, sets, width), bf16),
            pltpu.VMEM((n, nz, SUB, sets, width), bf16),
            pltpu.VMEM((n, nz, SUB, sets, width), bf16),
            pltpu.VMEM((n, half, pixels), bf16),
            pltpu.VMEM((n, half, pixels), bf16),
            pltpu.VMEM((n, npar, half, pixels), bf16),
            pltpu.VMEM((n, 2, sets, 2 * GRID), bf16),
            pltpu.VMEM((n + 1, nz, 1, 8, LANES), f32),
            pltpu.VMEM((n + 1, npar, 8, LANES), f32),
            pltpu.VMEM((n, nz, 1, 8, LANES), f32),
            pltpu.VMEM((n, npar, 8, LANES), f32),
            dma((nz, SUB)),
            dma((n, nz, SUB)), dma((n, nz, SUB)),
            dma((n, nz, SUB)), dma((n, nz, SUB)),
            dma((n,)), dma((n,)),
            dma((n, npar)), dma((n, npar)),
            dma((n, 2)), dma((n, 2)),
            dma((n + 1, nz, 1)), dma((n + 1, nz, 1)),
            dma((n + 1, npar)), dma((n + 1, npar)),
            dma((n, nz, 1)), dma((n, nz, 1)),
            dma((n, npar)), dma((n, npar)),
        ],
        compiler_params=pltpu.CompilerParams(
            collective_id=0, has_side_effects=True, vmem_limit_bytes=60 * 1024 * 1024
        ),
    )(green_matrix, observed)


def solution(mesh):
    nz, npar = mesh.shape["pix"], mesh.shape["par"]

    def step(green_matrix, observed):
        sets, cells = observed.shape[0], green_matrix.shape[1]
        width = cells // (nz * SUB)
        fits = cells % (nz * SUB * GRID) == 0 and width >= 2 * GRID and nz & (nz - 1) == 0
        if fits and nz > 1 and npar % 2 == 0 and sets % 32 == 0 and sets <= LANES:
            return on_device_kernel(nz, npar, green_matrix, observed)
        return on_device(green_matrix, observed)

    return jax.shard_map(
        step,
        mesh=mesh,
        in_specs=(P("pix", "par"), P("parts", "pix")),
        out_specs=(P("parts", "par"), P("parts", "pix")),
        check_vma=False,
    )
```

```python
import functools

import jax
import jax.numpy as jnp
from jax import lax
from jax.experimental import pallas as pl
from jax.experimental.pallas import tpu as pltpu
from jax.sharding import PartitionSpec as P

GRID = 128
ITERS = 5
LANES = 128
SUB = 2


def padded_2(block, sides, width):
    for axis, dim in sides:
        count = lax.axis_size(axis)
        forward = [(i, i + 1) for i in range(count - 1)]
        backward = [(target, source) for source, target in forward]
        low = lax.ppermute(
            lax.slice_in_dim(block, block.shape[dim] - width, None, axis=dim), axis, forward
        )
        high = lax.ppermute(lax.slice_in_dim(block, 0, width, axis=dim), axis, backward)
        block = jnp.concatenate([low, block, high], axis=dim)
    return block


def smooth(values):
    set_count = values.shape[0]
    grid_rows = values.shape[1] // GRID
    tiles = values.reshape(set_count, grid_rows, GRID)
    padded = padded_2(tiles, (("par", 1),), 1)
    padded = jnp.pad(padded, ((0, 0), (0, 0), (1, 1)))
    beside_all = (
        padded[:, 2:, 1:-1] + padded[:, :-2, 1:-1] + padded[:, 1:-1, 2:] + padded[:, 1:-1, :-2]
    )
    return (0.25 * (4.0 * tiles - beside_all)).reshape(set_count, grid_rows * GRID)


def forward(rounded, green_matrix):
    partial_value = lax.dot_general(
        rounded, green_matrix, (((1,), (1,)), ((), ())), preferred_element_type=jnp.float32
    )
    return lax.psum(partial_value, "par")


def curvatures(image, smoothed):
    local_image = jnp.sum(image * image, axis=1)
    local_smooth = jnp.sum(smoothed * smoothed, axis=1)
    image_sq = lax.psum(local_image, "pix")
    smooth_sq = lax.psum(local_smooth, "par")
    return image_sq + smooth_sq


def backward_sum(rounded, green_matrix):
    return lax.psum(jnp.dot(rounded, green_matrix, preferred_element_type=jnp.float32), "pix")


def column_squares(gradient):
    return lax.psum(jnp.sum(gradient * gradient, axis=1), "par")


def on_device(green_matrix, observed):
    set_count = observed.shape[0]
    tile_cells = green_matrix.shape[1]
    residual = observed.astype(jnp.float32)
    gradient = backward_sum(observed, green_matrix)
    grad_sq = column_squares(gradient)
    direction = gradient
    solution = jnp.zeros((set_count, tile_cells), jnp.float32)
    smooth_res = jnp.zeros((set_count, tile_cells), jnp.float32)
    for sweep in range(ITERS):
        rounded = direction.astype(jnp.bfloat16)
        image = forward(rounded, green_matrix)
        smoothed = smooth(lax.optimization_barrier(rounded).astype(jnp.float32))
        step_len = (grad_sq / curvatures(image, smoothed))[:, None]
        solution = solution + step_len * direction
        residual = residual - step_len * image
        smooth_res = smooth_res - step_len * smoothed
        if sweep + 1 < ITERS:
            gradient = backward_sum(residual.astype(jnp.bfloat16), green_matrix) + smooth(
                smooth_res
            )
            fresh_sq = column_squares(gradient)
            direction = gradient + (fresh_sq / grad_sq)[:, None] * direction
            grad_sq = fresh_sq
    return (solution, residual)


MESH = pl.DeviceIdType.MESH


def to_row(column):
    count = column.shape[0]
    eye = lax.broadcasted_iota(jnp.int32, (count, LANES), 0) == lax.broadcasted_iota(
        jnp.int32, (count, LANES), 1
    )
    return jnp.sum(jnp.where(eye, jnp.broadcast_to(column, (count, LANES)), 0.0), axis=0, keepdims=True)


def to_column(row, count):
    eye = lax.broadcasted_iota(jnp.int32, (count, LANES), 0) == lax.broadcasted_iota(
        jnp.int32, (count, LANES), 1
    )
    return jnp.sum(jnp.where(eye, jnp.broadcast_to(row, (count, LANES)), 0.0), axis=1, keepdims=True)


def flipped(index, mask, count):
    value, bit = 0, 1
    while bit < count:
        digit = lax.rem(index // bit, 2)
        value = value + bit * (1 - digit if mask & bit else digit)
        bit *= 2
    return value


def far_first(count):
    masks = []
    bit = count // 2
    while bit:
        masks += range(bit, 2 * bit)
        bit //= 2
    return masks


def stencil(above, here, below):
    lane = lax.broadcasted_iota(jnp.int32, here.shape, 1)
    left = jnp.where(lane == 0, 0.0, pltpu.roll(here, 1, 1))
    right = jnp.where(lane == GRID - 1, 0.0, pltpu.roll(here, GRID - 1, 1))
    return here - 0.25 * (above + below + left + right)


def cgls_kernel(
    nz, npar,
    green_hbm, obs_ref, x_ref, r_ref,
    green, imb, im, p_ext, sp, g_own, own_part, gg_ref,
    rs_send, rs_recv, ag, y_send, y_recv, h_recv, halo,
    sz, sp_scalar, nz_scalar, npar_scalar,
    load_sem, rs_ss, rs_rs, ag_ss, ag_rs, relay_ss, y_ss, y_rs, h_ss, h_rs, halo_ss, halo_rs,
    sz_ss, sz_rs, sp_ss, sp_rs, nz_ss, nz_rs, np_ss, np_rs,
):
    me_z = lax.axis_index("pix")
    me_p = lax.axis_index("par")
    core = lax.rem(me_p, 2)
    chip = me_p // 2
    nchip = npar // 2
    partner = me_p + 1 - 2 * core
    sets = obs_ref.shape[0]
    half = sets // 2
    width = green.shape[3]
    rows = nz * SUB * width // GRID
    own_rows = width // GRID
    edge = 2 * GRID
    z_peers = [flipped(me_z, mask, nz) for mask in far_first(nz)]
    z_from = z_peers[::-1]
    p_peers = [lax.rem(me_p + j, npar) for j in range(1, npar)]
    order = [(s, c) for s in range(SUB) for c in z_peers] + [(s, me_z) for s in range(SUB)]

    def load(s, c):
        first = pl.multiple_of((c * SUB + s) * width, width)
        return pltpu.make_async_copy(
            green_hbm.at[:, pl.ds(first, width)], green.at[c, s], load_sem.at[c, s]
        )

    for s, c in order:
        load(s, c).start()

    barrier = pltpu.get_barrier_semaphore()
    for j in range(1, nz):
        pl.semaphore_signal(barrier, inc=1, device_id={"pix": lax.rem(me_z + j, nz)}, device_id_type=MESH)
    for j in range(1, npar):
        pl.semaphore_signal(barrier, inc=1, device_id={"par": lax.rem(me_p + j, npar)}, device_id_type=MESH)

    imb[...] = obs_ref[...]
    im[...] = jnp.zeros_like(im)
    p_ext[...] = jnp.zeros_like(p_ext)
    g_own[...] = jnp.zeros_like(g_own)
    gg_ref[...] = jnp.zeros_like(gg_ref)
    x_ref[...] = jnp.zeros_like(x_ref)
    r_ref[...] = obs_ref[...].astype(jnp.float32)

    pl.semaphore_wait(barrier, nz + npar - 2)

    def to_z(buf, k, ssem, rsem, peer, s=0):
        return pltpu.make_async_remote_copy(
            src_ref=buf.at[k, me_z, s], dst_ref=buf.at[k, me_z, s],
            send_sem=ssem.at[k, peer, s], recv_sem=rsem.at[k, me_z, s],
            device_id={"pix": peer}, device_id_type=MESH,
        )

    def from_z(buf, k, ssem, rsem, peer, s=0):
        return pltpu.make_async_remote_copy(
            src_ref=buf.at[k, peer, s], dst_ref=buf.at[k, peer, s],
            send_sem=ssem.at[k, peer, s], recv_sem=rsem.at[k, peer, s],
            device_id={"pix": peer}, device_id_type=MESH,
        )

    def to_par(buf, k, ssem, rsem, peer):
        return pltpu.make_async_remote_copy(
            src_ref=buf.at[k, me_p], dst_ref=buf.at[k, me_p],
            send_sem=ssem.at[k, peer], recv_sem=rsem.at[k, me_p],
            device_id={"par": peer}, device_id_type=MESH,
        )

    def from_par(buf, k, ssem, rsem, peer):
        return pltpu.make_async_remote_copy(
            src_ref=buf.at[k, peer], dst_ref=buf.at[k, peer],
            send_sem=ssem.at[k, peer], recv_sem=rsem.at[k, peer],
            device_id={"par": peer}, device_id_type=MESH,
        )


    def total_row(parts):
        value = parts[0]
        for part in parts[1:]:
            value = value + part
        return value

    def z_row(buf, k):
        return total_row([buf[k, i, 0, 0:1] for i in range(nz)])

    def par_row(buf, k):
        return total_row([buf[k, i, 0:1] for i in range(npar)])

    def send_image_sq(k):
        image = im[...]
        row = to_row(jnp.sum(image * image, axis=1, keepdims=True))
        sz[k, me_z, 0] = jnp.broadcast_to(row, (8, LANES))
        for peer in z_peers:
            to_z(sz, k, sz_ss, sz_rs, peer).start()

    def send_smooth_sq(k):
        square = jnp.zeros((sets, GRID), jnp.float32)
        for i in range(rows + 2):
            line = stencil(
                p_ext[:, i * GRID:(i + 1) * GRID],
                p_ext[:, (i + 1) * GRID:(i + 2) * GRID],
                p_ext[:, (i + 2) * GRID:(i + 3) * GRID],
            )
            if i == 0:
                line = jnp.where(me_p == 0, 0.0, line)
            elif i == rows + 1:
                line = jnp.where(me_p == npar - 1, 0.0, line)
            else:
                square = square + line * line
            sp[:, i * GRID:(i + 1) * GRID] = line
        row = to_row(jnp.sum(square, axis=1, keepdims=True))
        sp_scalar[k, me_p] = jnp.broadcast_to(row, (8, LANES))
        for peer in p_peers:
            to_par(sp_scalar, k, sp_ss, sp_rs, peer).start()

    def curvature(k):
        for peer in p_peers:
            from_par(sp_scalar, k, sp_ss, sp_rs, peer).wait_recv()
        for peer in z_from:
            from_z(sz, k, sz_ss, sz_rs, peer).wait_recv()
        return z_row(sz, k) + par_row(sp_scalar, k)

    def apply_step(step):
        x_ref[...] += step * p_ext[:, edge:edge + rows * GRID]
        r_ref[...] -= step * im[...]

    def finish_scalars(k):
        for peer in z_peers:
            to_z(sz, k, sz_ss, sz_rs, peer).wait_send()
        for peer in p_peers:
            to_par(sp_scalar, k, sp_ss, sp_rs, peer).wait_send()

    def rs_copy(k, target, s):
        return pltpu.make_async_remote_copy(
            src_ref=rs_send.at[k, target, s], dst_ref=rs_recv.at[k, me_z, s],
            send_sem=rs_ss.at[k, target, s], recv_sem=rs_rs.at[k, me_z, s],
            device_id={"pix": target}, device_id_type=MESH,
        )

    def rs_from(k, source, s):
        return pltpu.make_async_remote_copy(
            src_ref=rs_send.at[k, source, s], dst_ref=rs_recv.at[k, source, s],
            send_sem=rs_ss.at[k, source, s], recv_sem=rs_rs.at[k, source, s],
            device_id={"pix": source}, device_id_type=MESH,
        )

    def relay_masks(s):
        if s + 1 == SUB:
            return []
        return [mask for mask in far_first(nz) if mask % 2 == 0]

    def sent_masks(s):
        if s + 1 == SUB:
            return far_first(nz)
        return [mask for mask in far_first(nz) if mask % 2 == 0 or mask == 1]

    def relay(k, source, s):
        mate = flipped(me_z, 1, nz)
        return pltpu.make_async_remote_copy(
            src_ref=ag.at[k, source, s], dst_ref=ag.at[k, source, s],
            send_sem=relay_ss.at[k, source, s], recv_sem=ag_rs.at[k, source, s],
            device_id={"pix": mate}, device_id_type=MESH,
        )

    up = lax.rem(me_p + 1, npar)
    down = lax.rem(me_p + npar - 1, npar)

    def halo_copies(k):
        return (
            pltpu.make_async_remote_copy(
                src_ref=ag.at[k, nz - 1, SUB - 1, :, pl.ds(width - edge, edge)], dst_ref=halo.at[k, 0],
                send_sem=halo_ss.at[k, 0], recv_sem=halo_rs.at[k, 0],
                device_id={"par": up}, device_id_type=MESH,
            ),
            pltpu.make_async_remote_copy(
                src_ref=ag.at[k, 0, 0, :, pl.ds(0, edge)], dst_ref=halo.at[k, 1],
                send_sem=halo_ss.at[k, 1], recv_sem=halo_rs.at[k, 1],
                device_id={"par": down}, device_id_type=MESH,
            ),
        )

    def y_copy(k):
        return pltpu.make_async_remote_copy(
            src_ref=y_send.at[k], dst_ref=y_recv.at[k],
            send_sem=y_ss.at[k], recv_sem=y_rs.at[k],
            device_id={"par": partner}, device_id_type=MESH,
        )

    @pl.loop(0, ITERS)
    def _(k):
        send_image_sq(k)
        vector = imb[...]

        def backward(s, c):
            @pl.when(k == 0)
            def _():
                load(s, c).wait()

            return jnp.dot(vector, green[c, s], preferred_element_type=jnp.float32)

        for s in range(SUB):
            for peer in z_peers:
                rs_send[k, peer, s] = backward(s, peer).astype(jnp.bfloat16)
                rs_copy(k, peer, s).start()
        send_smooth_sq(k)
        for s in range(SUB):
            base = (me_z * SUB + s) * own_rows
            lines = []
            for i in range(own_rows):
                lines.append(stencil(*[
                    sp[:, pl.ds(pl.multiple_of((base + i + d) * GRID, GRID), GRID)]
                    for d in range(3)
                ]))
            own_part[s] = backward(s, me_z) + jnp.concatenate(lines, axis=1)
        step = jnp.where(k == 0, -1.0, gg_ref[0:1] / curvature(k))
        step = to_column(step, sets)
        square = jnp.zeros((sets, 1), jnp.float32)
        for s in range(SUB):
            fresh = own_part[s]
            for source in z_from:
                rs_from(k, source, s).wait_recv()
                fresh = fresh + rs_recv[k, source, s].astype(jnp.float32)
            gradient = g_own[s] - step * fresh
            g_own[s] = gradient
            ag[k, me_z, s] = gradient.astype(jnp.bfloat16)
            for mask in sent_masks(s):
                to_z(ag, k, ag_ss, ag_rs, flipped(me_z, mask, nz), s).start()
            square = square + jnp.sum(gradient * gradient, axis=1, keepdims=True)
        nz_scalar[k, me_z, 0] = jnp.broadcast_to(to_row(square), (8, LANES))
        for peer in z_peers:
            to_z(nz_scalar, k, nz_ss, nz_rs, peer).start()
        apply_step(step)

        def forward(s, c):
            return lax.dot_general(
                ag[k, c, s], green[c, s], (((1,), (1,)), ((), ())),
                preferred_element_type=jnp.float32,
            )

        image = jnp.zeros(im.shape, jnp.float32)
        for s in range(SUB):
            image = image + forward(s, me_z)
        for s in range(SUB):
            for mask in relay_masks(s):
                source = flipped(me_z, mask, nz)
                from_z(ag, k, ag_ss, ag_rs, source, s).wait_recv()
                relay(k, source, s).start()
        for s in range(SUB):
            for mask in sent_masks(s)[::-1]:
                source = flipped(me_z, mask, nz)
                if mask not in relay_masks(s):
                    from_z(ag, k, ag_ss, ag_rs, source, s).wait_recv()
                image = image + forward(s, source)
            if s + 2 <= SUB:
                continue
            for t in range(SUB):
                for mask in relay_masks(t):
                    source = flipped(me_z, mask + 1, nz)
                    from_z(ag, k, ag_ss, ag_rs, source, t).wait_recv()
                    image = image + forward(t, source)
        low, high = image[:half], image[half:]
        mine = jnp.where(core == 0, low, high)
        y_send[k] = jnp.where(core == 0, high, low).astype(jnp.bfloat16)
        y_copy(k).start()
        for source in z_from:
            from_z(nz_scalar, k, nz_ss, nz_rs, source).wait_recv()
        npar_scalar[k, me_p] = jnp.broadcast_to(z_row(nz_scalar, k), (8, LANES))
        for peer in p_peers:
            to_par(npar_scalar, k, np_ss, np_rs, peer).start()
        for copy in halo_copies(k):
            copy.start()
        y_copy(k).wait_recv()
        h_recv[k, me_p] = (mine + y_recv[k].astype(jnp.float32)).astype(jnp.bfloat16)
        for peer in p_peers:
            to_par(h_recv, k, h_ss, h_rs, peer).start()

        for peer in p_peers:
            from_par(npar_scalar, k, np_ss, np_rs, peer).wait_recv()
        fresh_sq = par_row(npar_scalar, k)
        ratio = to_column(jnp.where(k == 0, 0.0, fresh_sq / gg_ref[0:1]), sets)
        gg_ref[...] = jnp.broadcast_to(fresh_sq, gg_ref.shape)
        for copy in halo_copies(k):
            copy.wait_recv()
        for c in range(nz):
            for s in range(SUB):
                first = edge + (c * SUB + s) * width
                where = slice(first, first + width)
                p_ext[:, where] = ag[k, c, s].astype(jnp.float32) + ratio * p_ext[:, where]
        first = jnp.where(me_p == 0, 0.0, halo[k, 0].astype(jnp.float32))
        p_ext[:, :edge] = first + ratio * p_ext[:, :edge]
        last = jnp.where(me_p == npar - 1, 0.0, halo[k, 1].astype(jnp.float32))
        p_ext[:, edge + rows * GRID:] = last + ratio * p_ext[:, edge + rows * GRID:]

        for peer in p_peers:
            from_par(h_recv, k, h_ss, h_rs, peer).wait_recv()
        for c in range(2):
            part = h_recv[k, c].astype(jnp.float32)
            for i in range(1, nchip):
                part = part + h_recv[k, 2 * i + c].astype(jnp.float32)
            where = slice(c * half, (c + 1) * half)
            im[where] = part + ratio[where] * im[where]
        imb[...] = im[...].astype(jnp.bfloat16)

        finish_scalars(k)
        for peer in z_peers:
            for s in range(SUB):
                rs_copy(k, peer, s).wait_send()
            to_z(nz_scalar, k, nz_ss, nz_rs, peer).wait_send()
        for s in range(SUB):
            for mask in sent_masks(s):
                to_z(ag, k, ag_ss, ag_rs, flipped(me_z, mask, nz), s).wait_send()
            for mask in relay_masks(s):
                relay(k, flipped(me_z, mask, nz), s).wait_send()
        y_copy(k).wait_send()
        for copy in halo_copies(k):
            copy.wait_send()
        for peer in p_peers:
            to_par(npar_scalar, k, np_ss, np_rs, peer).wait_send()
            to_par(h_recv, k, h_ss, h_rs, peer).wait_send()

    send_image_sq(ITERS)
    send_smooth_sq(ITERS)
    step = to_column(gg_ref[0:1] / curvature(ITERS), sets)
    apply_step(step)
    finish_scalars(ITERS)


def finish_kernel(x_ref, r_ref, x_out, r_out, x_sem, r_sem):
    copies = (
        pltpu.make_async_copy(x_ref, x_out, x_sem),
        pltpu.make_async_copy(r_ref, r_out, r_sem),
    )
    for copy in copies:
        copy.start()
    for copy in copies:
        copy.wait()


def finish(x, r):
    vmem = pl.BlockSpec(memory_space=pltpu.VMEM)
    space = pl.BlockSpec(memory_space=pl.ANY)
    return pl.pallas_call(
        finish_kernel,
        out_shape=(jax.ShapeDtypeStruct(x.shape, x.dtype), jax.ShapeDtypeStruct(r.shape, r.dtype)),
        in_specs=[vmem, vmem],
        out_specs=(space, space),
        scratch_shapes=[pltpu.SemaphoreType.DMA, pltpu.SemaphoreType.DMA],
    )(x, r)


def on_device_kernel(nz, npar, green_matrix, observed):
    sets, pixels = observed.shape
    cells = green_matrix.shape[1]
    width = cells // (nz * SUB)
    half = sets // 2
    bf16, f32 = jnp.bfloat16, jnp.float32
    dma = pltpu.SemaphoreType.DMA
    n = ITERS
    vmem = pl.BlockSpec(memory_space=pltpu.VMEM)
    return pl.pallas_call(
        functools.partial(cgls_kernel, nz, npar),
        out_shape=(
            jax.ShapeDtypeStruct((sets, cells), f32),
            jax.ShapeDtypeStruct((sets, pixels), f32),
        ),
        in_specs=[pl.BlockSpec(memory_space=pl.ANY), vmem],
        out_specs=(vmem, vmem),
        scratch_shapes=[
            pltpu.VMEM((nz, SUB, pixels, width), bf16),
            pltpu.VMEM((sets, pixels), bf16),
            pltpu.VMEM((sets, pixels), f32),
            pltpu.VMEM((sets, cells + 4 * GRID), f32),
            pltpu.VMEM((sets, cells + 2 * GRID), f32),
            pltpu.VMEM((SUB, sets, width), f32),
            pltpu.VMEM((SUB, sets, width), f32),
            pltpu.VMEM((8, LANES), f32),
            pltpu.VMEM((n, nz, SUB, sets, width), bf16),
            pltpu.VMEM((n, nz, SUB, sets, width), bf16),
            pltpu.VMEM((n, nz, SUB, sets, width), bf16),
            pltpu.VMEM((n, half, pixels), bf16),
            pltpu.VMEM((n, half, pixels), bf16),
            pltpu.VMEM((n, npar, half, pixels), bf16),
            pltpu.VMEM((n, 2, sets, 2 * GRID), bf16),
            pltpu.VMEM((n + 1, nz, 1, 8, LANES), f32),
            pltpu.VMEM((n + 1, npar, 8, LANES), f32),
            pltpu.VMEM((n, nz, 1, 8, LANES), f32),
            pltpu.VMEM((n, npar, 8, LANES), f32),
            dma((nz, SUB)),
            dma((n, nz, SUB)), dma((n, nz, SUB)),
            dma((n, nz, SUB)), dma((n, nz, SUB)),
            dma((n, nz, SUB)),
            dma((n,)), dma((n,)),
            dma((n, npar)), dma((n, npar)),
            dma((n, 2)), dma((n, 2)),
            dma((n + 1, nz, 1)), dma((n + 1, nz, 1)),
            dma((n + 1, npar)), dma((n + 1, npar)),
            dma((n, nz, 1)), dma((n, nz, 1)),
            dma((n, npar)), dma((n, npar)),
        ],
        compiler_params=pltpu.CompilerParams(
            collective_id=0, has_side_effects=True, vmem_limit_bytes=60 * 1024 * 1024
        ),
    )(green_matrix, observed)


def solution(mesh):
    nz, npar = mesh.shape["pix"], mesh.shape["par"]

    def step(green_matrix, observed):
        sets, cells = observed.shape[0], green_matrix.shape[1]
        width = cells // (nz * SUB)
        fits = cells % (nz * SUB * GRID) == 0 and width >= 2 * GRID and nz & (nz - 1) == 0
        if fits and nz > 1 and npar % 2 == 0 and sets % 32 == 0 and sets <= LANES:
            return finish(*on_device_kernel(nz, npar, green_matrix, observed))
        return on_device(green_matrix, observed)

    return jax.shard_map(
        step,
        mesh=mesh,
        in_specs=(P("pix", "par"), P("parts", "pix")),
        out_specs=(P("parts", "par"), P("parts", "pix")),
        check_vma=False,
    )
```

```python
import functools

import jax
import jax.numpy as jnp
from jax import lax
from jax.experimental import pallas as pl
from jax.experimental.pallas import tpu as pltpu
from jax.sharding import PartitionSpec as P

GRID = 128
ITERS = 5
LANES = 128
SUB = 2


def padded_2(block, sides, width):
    for axis, dim in sides:
        count = lax.axis_size(axis)
        forward = [(i, i + 1) for i in range(count - 1)]
        backward = [(target, source) for source, target in forward]
        low = lax.ppermute(
            lax.slice_in_dim(block, block.shape[dim] - width, None, axis=dim), axis, forward
        )
        high = lax.ppermute(lax.slice_in_dim(block, 0, width, axis=dim), axis, backward)
        block = jnp.concatenate([low, block, high], axis=dim)
    return block


def smooth(values):
    set_count = values.shape[0]
    grid_rows = values.shape[1] // GRID
    tiles = values.reshape(set_count, grid_rows, GRID)
    padded = padded_2(tiles, (("par", 1),), 1)
    padded = jnp.pad(padded, ((0, 0), (0, 0), (1, 1)))
    beside_all = (
        padded[:, 2:, 1:-1] + padded[:, :-2, 1:-1] + padded[:, 1:-1, 2:] + padded[:, 1:-1, :-2]
    )
    return (0.25 * (4.0 * tiles - beside_all)).reshape(set_count, grid_rows * GRID)


def forward(rounded, green_matrix):
    partial_value = lax.dot_general(
        rounded, green_matrix, (((1,), (1,)), ((), ())), preferred_element_type=jnp.float32
    )
    return lax.psum(partial_value, "par")


def curvatures(image, smoothed):
    local_image = jnp.sum(image * image, axis=1)
    local_smooth = jnp.sum(smoothed * smoothed, axis=1)
    image_sq = lax.psum(local_image, "pix")
    smooth_sq = lax.psum(local_smooth, "par")
    return image_sq + smooth_sq


def backward_sum(rounded, green_matrix):
    return lax.psum(jnp.dot(rounded, green_matrix, preferred_element_type=jnp.float32), "pix")


def column_squares(gradient):
    return lax.psum(jnp.sum(gradient * gradient, axis=1), "par")


def on_device(green_matrix, observed):
    set_count = observed.shape[0]
    tile_cells = green_matrix.shape[1]
    residual = observed.astype(jnp.float32)
    gradient = backward_sum(observed, green_matrix)
    grad_sq = column_squares(gradient)
    direction = gradient
    solution = jnp.zeros((set_count, tile_cells), jnp.float32)
    smooth_res = jnp.zeros((set_count, tile_cells), jnp.float32)
    for sweep in range(ITERS):
        rounded = direction.astype(jnp.bfloat16)
        image = forward(rounded, green_matrix)
        smoothed = smooth(lax.optimization_barrier(rounded).astype(jnp.float32))
        step_len = (grad_sq / curvatures(image, smoothed))[:, None]
        solution = solution + step_len * direction
        residual = residual - step_len * image
        smooth_res = smooth_res - step_len * smoothed
        if sweep + 1 < ITERS:
            gradient = backward_sum(residual.astype(jnp.bfloat16), green_matrix) + smooth(
                smooth_res
            )
            fresh_sq = column_squares(gradient)
            direction = gradient + (fresh_sq / grad_sq)[:, None] * direction
            grad_sq = fresh_sq
    return (solution, residual)


MESH = pl.DeviceIdType.MESH


def to_row(column):
    count = column.shape[0]
    eye = lax.broadcasted_iota(jnp.int32, (count, LANES), 0) == lax.broadcasted_iota(
        jnp.int32, (count, LANES), 1
    )
    return jnp.sum(jnp.where(eye, jnp.broadcast_to(column, (count, LANES)), 0.0), axis=0, keepdims=True)


def to_column(row, count):
    eye = lax.broadcasted_iota(jnp.int32, (count, LANES), 0) == lax.broadcasted_iota(
        jnp.int32, (count, LANES), 1
    )
    return jnp.sum(jnp.where(eye, jnp.broadcast_to(row, (count, LANES)), 0.0), axis=1, keepdims=True)


def flipped(index, mask, count):
    value, bit = 0, 1
    while bit < count:
        digit = lax.rem(index // bit, 2)
        value = value + bit * (1 - digit if mask & bit else digit)
        bit *= 2
    return value


def far_first(count):
    masks = []
    bit = count // 2
    while bit:
        masks += range(bit, 2 * bit)
        bit //= 2
    return masks


def stencil(above, here, below):
    lane = lax.broadcasted_iota(jnp.int32, here.shape, 1)
    left = jnp.where(lane == 0, 0.0, pltpu.roll(here, 1, 1))
    right = jnp.where(lane == GRID - 1, 0.0, pltpu.roll(here, GRID - 1, 1))
    return here - 0.25 * (above + below + left + right)


def cgls_kernel(
    nz, npar,
    green_hbm, obs_ref, x_ref, r_ref,
    green, imb, im, p_ext, sp, g_own, own_part, gg_ref,
    rs_send, rs_recv, ag, y_send, y_recv, h_recv, halo,
    sz, sp_scalar, nz_scalar, npar_scalar,
    load_sem, rs_ss, rs_rs, ag_ss, ag_rs, relay_ss, y_ss, y_rs, h_ss, h_rs, halo_ss, halo_rs,
    sz_ss, sz_rs, sp_ss, sp_rs, nz_ss, nz_rs, np_ss, np_rs,
):
    me_z = lax.axis_index("pix")
    me_p = lax.axis_index("par")
    core = lax.rem(me_p, 2)
    chip = me_p // 2
    nchip = npar // 2
    partner = me_p + 1 - 2 * core
    sets = obs_ref.shape[0]
    half = sets // 2
    width = green.shape[3]
    rows = nz * SUB * width // GRID
    own_rows = width // GRID
    edge = 2 * GRID
    z_peers = [flipped(me_z, mask, nz) for mask in far_first(nz)]
    z_from = z_peers[::-1]
    p_peers = [lax.rem(me_p + j, npar) for j in range(1, npar)]
    order = [(s, c) for s in range(SUB) for c in z_peers] + [(s, me_z) for s in range(SUB)]

    def load(s, c):
        first = pl.multiple_of((c * SUB + s) * width, width)
        return pltpu.make_async_copy(
            green_hbm.at[:, pl.ds(first, width)], green.at[c, s], load_sem.at[c, s]
        )

    for s, c in order:
        load(s, c).start()

    barrier = pltpu.get_barrier_semaphore()
    for j in range(1, nz):
        pl.semaphore_signal(barrier, inc=1, device_id={"pix": lax.rem(me_z + j, nz)}, device_id_type=MESH)
    for j in range(1, npar):
        pl.semaphore_signal(barrier, inc=1, device_id={"par": lax.rem(me_p + j, npar)}, device_id_type=MESH)

    imb[...] = obs_ref[...]
    im[...] = jnp.zeros_like(im)
    p_ext[...] = jnp.zeros_like(p_ext)
    g_own[...] = jnp.zeros_like(g_own)
    gg_ref[...] = jnp.zeros_like(gg_ref)
    x_ref[...] = jnp.zeros_like(x_ref)
    r_ref[...] = obs_ref[...].astype(jnp.float32)

    pl.semaphore_wait(barrier, nz + npar - 2)

    def to_z(buf, k, ssem, rsem, peer, s=0):
        return pltpu.make_async_remote_copy(
            src_ref=buf.at[k, me_z, s], dst_ref=buf.at[k, me_z, s],
            send_sem=ssem.at[k, peer, s], recv_sem=rsem.at[k, me_z, s],
            device_id={"pix": peer}, device_id_type=MESH,
        )

    def from_z(buf, k, ssem, rsem, peer, s=0):
        return pltpu.make_async_remote_copy(
            src_ref=buf.at[k, peer, s], dst_ref=buf.at[k, peer, s],
            send_sem=ssem.at[k, peer, s], recv_sem=rsem.at[k, peer, s],
            device_id={"pix": peer}, device_id_type=MESH,
        )

    def to_par(buf, k, ssem, rsem, peer):
        return pltpu.make_async_remote_copy(
            src_ref=buf.at[k, me_p], dst_ref=buf.at[k, me_p],
            send_sem=ssem.at[k, peer], recv_sem=rsem.at[k, me_p],
            device_id={"par": peer}, device_id_type=MESH,
        )

    def from_par(buf, k, ssem, rsem, peer):
        return pltpu.make_async_remote_copy(
            src_ref=buf.at[k, peer], dst_ref=buf.at[k, peer],
            send_sem=ssem.at[k, peer], recv_sem=rsem.at[k, peer],
            device_id={"par": peer}, device_id_type=MESH,
        )


    def total_row(parts):
        value = parts[0]
        for part in parts[1:]:
            value = value + part
        return value

    def z_row(buf, k):
        return total_row([buf[k, i, 0, 0:1] for i in range(nz)])

    def par_row(buf, k):
        return total_row([buf[k, i, 0:1] for i in range(npar)])

    def send_image_sq(k):
        image = im[...]
        row = to_row(jnp.sum(image * image, axis=1, keepdims=True))
        sz[k, me_z, 0] = jnp.broadcast_to(row, (8, LANES))
        for peer in z_peers:
            to_z(sz, k, sz_ss, sz_rs, peer).start()

    def send_smooth_sq(k):
        square = jnp.zeros((sets, GRID), jnp.float32)
        for i in range(rows + 2):
            line = stencil(
                p_ext[:, i * GRID:(i + 1) * GRID],
                p_ext[:, (i + 1) * GRID:(i + 2) * GRID],
                p_ext[:, (i + 2) * GRID:(i + 3) * GRID],
            )
            if i == 0:
                line = jnp.where(me_p == 0, 0.0, line)
            elif i == rows + 1:
                line = jnp.where(me_p == npar - 1, 0.0, line)
            else:
                square = square + line * line
            sp[:, i * GRID:(i + 1) * GRID] = line
        row = to_row(jnp.sum(square, axis=1, keepdims=True))
        sp_scalar[k, me_p] = jnp.broadcast_to(row, (8, LANES))
        for peer in p_peers:
            to_par(sp_scalar, k, sp_ss, sp_rs, peer).start()

    def curvature(k):
        for peer in p_peers:
            from_par(sp_scalar, k, sp_ss, sp_rs, peer).wait_recv()
        for peer in z_from:
            from_z(sz, k, sz_ss, sz_rs, peer).wait_recv()
        return z_row(sz, k) + par_row(sp_scalar, k)

    def apply_step(step):
        x_ref[...] += step * p_ext[:, edge:edge + rows * GRID]
        r_ref[...] -= step * im[...]

    def finish_scalars(k):
        for peer in z_peers:
            to_z(sz, k, sz_ss, sz_rs, peer).wait_send()
        for peer in p_peers:
            to_par(sp_scalar, k, sp_ss, sp_rs, peer).wait_send()

    def rs_copy(k, target, s):
        return pltpu.make_async_remote_copy(
            src_ref=rs_send.at[k, target, s], dst_ref=rs_recv.at[k, me_z, s],
            send_sem=rs_ss.at[k, target, s], recv_sem=rs_rs.at[k, me_z, s],
            device_id={"pix": target}, device_id_type=MESH,
        )

    def rs_from(k, source, s):
        return pltpu.make_async_remote_copy(
            src_ref=rs_send.at[k, source, s], dst_ref=rs_recv.at[k, source, s],
            send_sem=rs_ss.at[k, source, s], recv_sem=rs_rs.at[k, source, s],
            device_id={"pix": source}, device_id_type=MESH,
        )

    def relay_masks(s):
        if s + 1 == SUB:
            return []
        return [mask for mask in far_first(nz) if mask % 2 == 0]

    def sent_masks(s):
        if s + 1 == SUB:
            return far_first(nz)
        return [mask for mask in far_first(nz) if mask % 2 == 0 or mask == 1]

    def relay(k, source, s):
        mate = flipped(me_z, 1, nz)
        return pltpu.make_async_remote_copy(
            src_ref=ag.at[k, source, s], dst_ref=ag.at[k, source, s],
            send_sem=relay_ss.at[k, source, s], recv_sem=ag_rs.at[k, source, s],
            device_id={"pix": mate}, device_id_type=MESH,
        )

    up = lax.rem(me_p + 1, npar)
    down = lax.rem(me_p + npar - 1, npar)

    def halo_copies(k):
        return (
            pltpu.make_async_remote_copy(
                src_ref=ag.at[k, nz - 1, SUB - 1, :, pl.ds(width - edge, edge)], dst_ref=halo.at[k, 0],
                send_sem=halo_ss.at[k, 0], recv_sem=halo_rs.at[k, 0],
                device_id={"par": up}, device_id_type=MESH,
            ),
            pltpu.make_async_remote_copy(
                src_ref=ag.at[k, 0, 0, :, pl.ds(0, edge)], dst_ref=halo.at[k, 1],
                send_sem=halo_ss.at[k, 1], recv_sem=halo_rs.at[k, 1],
                device_id={"par": down}, device_id_type=MESH,
            ),
        )

    def y_copy(k):
        return pltpu.make_async_remote_copy(
            src_ref=y_send.at[k], dst_ref=y_recv.at[k],
            send_sem=y_ss.at[k], recv_sem=y_rs.at[k],
            device_id={"par": partner}, device_id_type=MESH,
        )

    @pl.loop(0, ITERS)
    def _(k):
        send_image_sq(k)
        vector = imb[...]

        def backward(s, c):
            @pl.when(k == 0)
            def _():
                load(s, c).wait()

            return jnp.dot(vector, green[c, s], preferred_element_type=jnp.float32)

        for s in range(SUB):
            for peer in z_peers:
                rs_send[k, peer, s] = backward(s, peer).astype(jnp.bfloat16)
                rs_copy(k, peer, s).start()
        send_smooth_sq(k)
        for s in range(SUB):
            base = (me_z * SUB + s) * own_rows
            lines = []
            for i in range(own_rows):
                lines.append(stencil(*[
                    sp[:, pl.ds(pl.multiple_of((base + i + d) * GRID, GRID), GRID)]
                    for d in range(3)
                ]))
            own_part[s] = backward(s, me_z) + jnp.concatenate(lines, axis=1)
        step = jnp.where(k == 0, -1.0, gg_ref[0:1] / curvature(k))
        step = to_column(step, sets)
        square = jnp.zeros((sets, 1), jnp.float32)
        for s in range(SUB):
            fresh = own_part[s]
            for source in z_from:
                rs_from(k, source, s).wait_recv()
                fresh = fresh + rs_recv[k, source, s].astype(jnp.float32)
            gradient = g_own[s] - step * fresh
            g_own[s] = gradient
            ag[k, me_z, s] = gradient.astype(jnp.bfloat16)
            for mask in sent_masks(s):
                to_z(ag, k, ag_ss, ag_rs, flipped(me_z, mask, nz), s).start()
            square = square + jnp.sum(gradient * gradient, axis=1, keepdims=True)
        nz_scalar[k, me_z, 0] = jnp.broadcast_to(to_row(square), (8, LANES))
        for peer in z_peers:
            to_z(nz_scalar, k, nz_ss, nz_rs, peer).start()
        apply_step(step)

        def forward(s, c):
            return lax.dot_general(
                ag[k, c, s], green[c, s], (((1,), (1,)), ((), ())),
                preferred_element_type=jnp.float32,
            )

        image = jnp.zeros(im.shape, jnp.float32)
        for s in range(SUB):
            image = image + forward(s, me_z)
        for s in range(SUB):
            for mask in relay_masks(s):
                source = flipped(me_z, mask, nz)
                from_z(ag, k, ag_ss, ag_rs, source, s).wait_recv()
                relay(k, source, s).start()
        for s in range(SUB):
            for mask in sent_masks(s)[::-1]:
                source = flipped(me_z, mask, nz)
                if s + 1 == SUB and mask == nz // 2:
                    for t in range(SUB):
                        for held in relay_masks(t):
                            distant = flipped(me_z, held + 1, nz)
                            from_z(ag, k, ag_ss, ag_rs, distant, t).wait_recv()
                            image = image + forward(t, distant)
                if mask not in relay_masks(s):
                    from_z(ag, k, ag_ss, ag_rs, source, s).wait_recv()
                image = image + forward(s, source)
        low, high = image[:half], image[half:]
        mine = jnp.where(core == 0, low, high)
        y_send[k] = jnp.where(core == 0, high, low).astype(jnp.bfloat16)
        y_copy(k).start()
        for source in z_from:
            from_z(nz_scalar, k, nz_ss, nz_rs, source).wait_recv()
        npar_scalar[k, me_p] = jnp.broadcast_to(z_row(nz_scalar, k), (8, LANES))
        for peer in p_peers:
            to_par(npar_scalar, k, np_ss, np_rs, peer).start()
        for copy in halo_copies(k):
            copy.start()
        y_copy(k).wait_recv()
        h_recv[k, me_p] = (mine + y_recv[k].astype(jnp.float32)).astype(jnp.bfloat16)
        for peer in p_peers:
            to_par(h_recv, k, h_ss, h_rs, peer).start()

        for peer in p_peers:
            from_par(npar_scalar, k, np_ss, np_rs, peer).wait_recv()
        fresh_sq = par_row(npar_scalar, k)
        ratio = to_column(jnp.where(k == 0, 0.0, fresh_sq / gg_ref[0:1]), sets)
        gg_ref[...] = jnp.broadcast_to(fresh_sq, gg_ref.shape)
        for copy in halo_copies(k):
            copy.wait_recv()
        for c in range(nz):
            for s in range(SUB):
                first = edge + (c * SUB + s) * width
                where = slice(first, first + width)
                p_ext[:, where] = ag[k, c, s].astype(jnp.float32) + ratio * p_ext[:, where]
        first = jnp.where(me_p == 0, 0.0, halo[k, 0].astype(jnp.float32))
        p_ext[:, :edge] = first + ratio * p_ext[:, :edge]
        last = jnp.where(me_p == npar - 1, 0.0, halo[k, 1].astype(jnp.float32))
        p_ext[:, edge + rows * GRID:] = last + ratio * p_ext[:, edge + rows * GRID:]

        for peer in p_peers:
            from_par(h_recv, k, h_ss, h_rs, peer).wait_recv()
        for c in range(2):
            part = h_recv[k, c].astype(jnp.float32)
            for i in range(1, nchip):
                part = part + h_recv[k, 2 * i + c].astype(jnp.float32)
            where = slice(c * half, (c + 1) * half)
            im[where] = part + ratio[where] * im[where]
        imb[...] = im[...].astype(jnp.bfloat16)

        finish_scalars(k)
        for peer in z_peers:
            for s in range(SUB):
                rs_copy(k, peer, s).wait_send()
            to_z(nz_scalar, k, nz_ss, nz_rs, peer).wait_send()
        for s in range(SUB):
            for mask in sent_masks(s):
                to_z(ag, k, ag_ss, ag_rs, flipped(me_z, mask, nz), s).wait_send()
            for mask in relay_masks(s):
                relay(k, flipped(me_z, mask, nz), s).wait_send()
        y_copy(k).wait_send()
        for copy in halo_copies(k):
            copy.wait_send()
        for peer in p_peers:
            to_par(npar_scalar, k, np_ss, np_rs, peer).wait_send()
            to_par(h_recv, k, h_ss, h_rs, peer).wait_send()

    send_image_sq(ITERS)
    send_smooth_sq(ITERS)
    step = to_column(gg_ref[0:1] / curvature(ITERS), sets)
    apply_step(step)
    finish_scalars(ITERS)


def finish_kernel(x_ref, r_ref, x_out, r_out, x_sem, r_sem):
    copies = (
        pltpu.make_async_copy(x_ref, x_out, x_sem),
        pltpu.make_async_copy(r_ref, r_out, r_sem),
    )
    for copy in copies:
        copy.start()
    for copy in copies:
        copy.wait()


def finish(x, r):
    vmem = pl.BlockSpec(memory_space=pltpu.VMEM)
    space = pl.BlockSpec(memory_space=pl.ANY)
    return pl.pallas_call(
        finish_kernel,
        out_shape=(jax.ShapeDtypeStruct(x.shape, x.dtype), jax.ShapeDtypeStruct(r.shape, r.dtype)),
        in_specs=[vmem, vmem],
        out_specs=(space, space),
        scratch_shapes=[pltpu.SemaphoreType.DMA, pltpu.SemaphoreType.DMA],
    )(x, r)


def on_device_kernel(nz, npar, green_matrix, observed):
    sets, pixels = observed.shape
    cells = green_matrix.shape[1]
    width = cells // (nz * SUB)
    half = sets // 2
    bf16, f32 = jnp.bfloat16, jnp.float32
    dma = pltpu.SemaphoreType.DMA
    n = ITERS
    vmem = pl.BlockSpec(memory_space=pltpu.VMEM)
    return pl.pallas_call(
        functools.partial(cgls_kernel, nz, npar),
        out_shape=(
            jax.ShapeDtypeStruct((sets, cells), f32),
            jax.ShapeDtypeStruct((sets, pixels), f32),
        ),
        in_specs=[pl.BlockSpec(memory_space=pl.ANY), vmem],
        out_specs=(vmem, vmem),
        scratch_shapes=[
            pltpu.VMEM((nz, SUB, pixels, width), bf16),
            pltpu.VMEM((sets, pixels), bf16),
            pltpu.VMEM((sets, pixels), f32),
            pltpu.VMEM((sets, cells + 4 * GRID), f32),
            pltpu.VMEM((sets, cells + 2 * GRID), f32),
            pltpu.VMEM((SUB, sets, width), f32),
            pltpu.VMEM((SUB, sets, width), f32),
            pltpu.VMEM((8, LANES), f32),
            pltpu.VMEM((n, nz, SUB, sets, width), bf16),
            pltpu.VMEM((n, nz, SUB, sets, width), bf16),
            pltpu.VMEM((n, nz, SUB, sets, width), bf16),
            pltpu.VMEM((n, half, pixels), bf16),
            pltpu.VMEM((n, half, pixels), bf16),
            pltpu.VMEM((n, npar, half, pixels), bf16),
            pltpu.VMEM((n, 2, sets, 2 * GRID), bf16),
            pltpu.VMEM((n + 1, nz, 1, 8, LANES), f32),
            pltpu.VMEM((n + 1, npar, 8, LANES), f32),
            pltpu.VMEM((n, nz, 1, 8, LANES), f32),
            pltpu.VMEM((n, npar, 8, LANES), f32),
            dma((nz, SUB)),
            dma((n, nz, SUB)), dma((n, nz, SUB)),
            dma((n, nz, SUB)), dma((n, nz, SUB)),
            dma((n, nz, SUB)),
            dma((n,)), dma((n,)),
            dma((n, npar)), dma((n, npar)),
            dma((n, 2)), dma((n, 2)),
            dma((n + 1, nz, 1)), dma((n + 1, nz, 1)),
            dma((n + 1, npar)), dma((n + 1, npar)),
            dma((n, nz, 1)), dma((n, nz, 1)),
            dma((n, npar)), dma((n, npar)),
        ],
        compiler_params=pltpu.CompilerParams(
            collective_id=0, has_side_effects=True, vmem_limit_bytes=60 * 1024 * 1024
        ),
    )(green_matrix, observed)


def solution(mesh):
    nz, npar = mesh.shape["pix"], mesh.shape["par"]

    def step(green_matrix, observed):
        sets, cells = observed.shape[0], green_matrix.shape[1]
        width = cells // (nz * SUB)
        fits = cells % (nz * SUB * GRID) == 0 and width >= 2 * GRID and nz & (nz - 1) == 0
        if fits and nz > 1 and npar % 2 == 0 and sets % 32 == 0 and sets <= LANES:
            return finish(*on_device_kernel(nz, npar, green_matrix, observed))
        return on_device(green_matrix, observed)

    return jax.shard_map(
        step,
        mesh=mesh,
        in_specs=(P("pix", "par"), P("parts", "pix")),
        out_specs=(P("parts", "par"), P("parts", "pix")),
        check_vma=False,
    )
```
